32 devices in a mesh: gx: 8 (over y, x, core), gy: 4 (over z).
Axes of the slice: x: 2, y: 2, z: 4, core: 2. Of those that a mesh axis runs over, the one named last changes fastest.
Arguments:
- cost: float32 [16, 1024, 512], P(None, 'gx', 'gy'), may hold values from 0 to 7.5
- density_start: float32 [16, 1024, 512], P(None, 'gx', 'gy'), may hold values from 0.125 to 4.5
- coupling: float32 [16, 16], replicated, may hold values from 0 to 0.25
Outputs:
- value: float32 [16, 1024, 512], P(None, 'gx', 'gy')
- density: float32 [16, 1024, 512], P(None, 'gx', 'gy')
- ergodic: float32 [16], replicated
The draws below stay inside these ranges and needn't reach their ends.
All inputs are finite; a program needn't handle non-finite values.
Results may differ from the reference program's by a relative error of at most 0.0003.
Values sent between devices are 32-bit elements; how exact they have to be, the bound alone decides.
A program may use at most 64 MiB of HBM per device.

```python
import jax
import jax.numpy as jnp
from jax import lax

K = 16
PICARD = 1
SWEEPS = 5
NX = 1024
NY = 512


def draw_cost(key, part):
    rows = jnp.arange(NX, dtype=jnp.float32) / NX
    cols = jnp.arange(NY, dtype=jnp.float32) / NY
    ramp = 0.5 + rows[:, None] + cols[None, :]
    base = jax.random.uniform(key, (K, NX, NY), jnp.float32, 0.0, 2.0)
    return base * ramp[None]


def draw_density_start(key, part):
    rows = jnp.arange(NX, dtype=jnp.float32) / NX
    cols = jnp.arange(NY, dtype=jnp.float32) / NY
    ramp = (0.5 + rows[:, None]) * (0.5 + cols[None, :])
    base = jax.random.uniform(key, (K, NX, NY), jnp.float32, 0.5, 2.0)
    return base * ramp[None]


def setup_inputs(seed: int = 0) -> dict:
    arg_keys = jax.random.split(jax.random.key(seed), 4)
    cost = draw_cost(jax.random.fold_in(arg_keys[3], 71), 0)
    density_start = draw_density_start(jax.random.fold_in(arg_keys[3], 71), 0)
    coupling = jnp.clip(jax.random.uniform(arg_keys[2], (K, K), jnp.float32, 0.0, 0.25), 0.0, 0.25)
    return dict(cost=cost, density_start=density_start, coupling=coupling)


viscosity = 0.5
theta = 2.0


def rates(u):
    u_xp = jnp.roll(u, -1, axis=0)
    u_xm = jnp.roll(u, 1, axis=0)
    u_yp = jnp.roll(u, -1, axis=1)
    u_ym = jnp.roll(u, 1, axis=1)
    vx = -(u_xp - u_xm) * 0.5
    vy = -(u_yp - u_ym) * 0.5
    r_xp = viscosity + jnp.maximum(vx, 0.0)
    r_xm = viscosity + jnp.maximum(-vx, 0.0)
    r_yp = viscosity + jnp.maximum(vy, 0.0)
    r_ym = viscosity + jnp.maximum(-vy, 0.0)
    total = r_xp + r_xm + r_yp + r_ym
    speed = (vx * vx + vy * vy) * 0.5
    return (r_xp, r_xm, r_yp, r_ym), (u_xp, u_xm, u_yp, u_ym), total, speed


def one_class(items):
    source, value, density, lam = items
    for sweep in range(SWEEPS):
        (r_xp, r_xm, r_yp, r_ym), (u_xp, u_xm, u_yp, u_ym), total, speed = rates(value)
        trial = (source + speed - lam + r_xp * u_xp + r_xm * u_xm + r_yp * u_yp + r_ym * u_ym) / total
        shift = jnp.mean(trial)
        lam = lam + theta * shift
        value = trial - shift
    (r_xp, r_xm, r_yp, r_ym), unused, total, speed = rates(value)
    c_xp = jnp.roll(r_xm, -1, axis=0) / total
    c_xm = jnp.roll(r_xp, 1, axis=0) / total
    c_yp = jnp.roll(r_ym, -1, axis=1) / total
    c_ym = jnp.roll(r_yp, 1, axis=1) / total
    for sweep in range(SWEEPS):
        fresh = (c_xp * jnp.roll(density, -1, axis=0) + c_xm * jnp.roll(density, 1, axis=0)
                 + c_yp * jnp.roll(density, -1, axis=1) + c_ym * jnp.roll(density, 1, axis=1))
        density = fresh / jnp.mean(fresh)
    return value, density, lam


def reference(cost, density_start, coupling):
    value = jnp.zeros(cost.shape, jnp.float32)
    density = density_start
    ergodic = jnp.zeros((cost.shape[0],), jnp.float32)
    for picard in range(PICARD):
        source = cost + jnp.einsum("kj,jxy->kxy", coupling, density, precision=lax.Precision.HIGHEST)
        value, density, ergodic = lax.map(one_class, (source, value, density, ergodic))
    return value, density, ergodic
```

```python
import functools

import jax
import jax.numpy as jnp
from jax import lax
from jax.experimental import pallas as pl
from jax.experimental.pallas import tpu as pltpu
from jax.sharding import PartitionSpec as P

MESH = pl.DeviceIdType.MESH
SWEEPS = 5
THETA = 2.0
PAD = 8
CHUNK = 32
UNROLL = 2


def kernel(
    nx, ny,
    cost_hbm, dens_hbm, coupling,
    trial_hbm, fresh_hbm, means,
    src, u, a, b, d0, d1, cxp, cxm, cyp, cym,
    xs, xr, ps, pr, xs2, xr2, ps2, pr2, edge, edge2,
    ar_out, ar_in, lam_tab,
    in_sem, out_sem, hs_sem, hr_sem, as_sem, ar_sem,
):
    classes, rows, cols = cost_hbm.shape
    n = nx * ny
    cells = float(n * rows * cols)
    gx, gy = lax.axis_index("gx"), lax.axis_index("gy")
    me = gx * ny + gy
    up, down = lax.rem(gx + nx - 1, nx), lax.rem(gx + 1, nx)
    left, right = lax.rem(gy + ny - 1, ny), lax.rem(gy + 1, ny)

    def at(x, y):
        return {"gx": x, "gy": y}

    def device(d):
        t = lax.rem(me + d, n)
        return at(t // ny, lax.rem(t, ny))

    load_d = pltpu.make_async_copy(dens_hbm, d0.at[:, pl.ds(PAD, rows), :], in_sem.at[0])
    load_c = pltpu.make_async_copy(cost_hbm, src, in_sem.at[1])
    load_d.start()
    load_c.start()

    barrier = pltpu.get_barrier_semaphore()

    def greet(d, carry):
        pl.semaphore_signal(barrier, inc=1, device_id=device(d), device_id_type=MESH)
        return carry

    lax.fori_loop(1, n, greet, 0)

    lane = lax.broadcasted_iota(jnp.int32, (1, cols), 1)
    lane_c = lax.broadcasted_iota(jnp.int32, (CHUNK, cols), 1)

    def geometry(w):
        span = 2 * w * classes
        return span, rows // (cols // span)

    def pack(ref, t, k, r0, w):
        span, block = geometry(w)
        p = span * (r0 // block) + 2 * w * k
        q = r0 % block
        turned = pltpu.roll(t, p + w, 1)
        mine = (lane_c >= p) & (lane_c < p + 2 * w)
        ref[q:q + CHUNK, :] = jnp.where(mine, turned, ref[q:q + CHUNK, :])

    def unpack(ref, k, r0, w):
        span, block = geometry(w)
        p = span * (r0 // block) + 2 * w * k
        q = r0 % block
        return pltpu.roll(ref[q:q + CHUNK, :], lax.rem(2 * cols - p, cols), 1)

    def halo_copies(e, w):
        sx, rx, sp, rp = (xs.at[e], xr.at[e], ps.at[e], pr.at[e]) if w == 1 else (xs2, xr2, ps2, pr2)
        plan = (
            (sx.at[0], rx.at[1], at(up, gy)),
            (sx.at[1], rx.at[0], at(down, gy)),
            (sp, rp.at[0], at(gx, right)),
            (sp, rp.at[1], at(gx, left)),
        )
        return [
            pltpu.make_async_remote_copy(
                src_ref=s, dst_ref=r, send_sem=hs_sem.at[e, i], recv_sem=hr_sem.at[e, i],
                device_id=dev, device_id_type=MESH,
            )
            for i, (s, r, dev) in enumerate(plan)
        ]

    def send_halo(e, w):
        copies = halo_copies(e, w)
        for c in copies:
            c.start()
        return copies

    def take_halo(copies, e, w, field):
        for c in copies:
            c.wait_recv()
        rx, rp, ed = (xr.at[e], pr.at[e], edge) if w == 1 else (xr2, pr2, edge2)
        for k in range(classes):
            for j in range(w):
                field[k, PAD - w + j:PAD - w + j + 1, :] = rx[0, j, k:k + 1, :]
                field[k, PAD + rows + j:PAD + rows + j + 1, :] = rx[1, j, k:k + 1, :]
        size = ed.shape[0]
        lanes = lax.broadcasted_iota(jnp.int32, (size, cols), 1)
        ed[...] = jnp.where(
            lax.rem(lanes, 2 * w) < w, rp[0], pltpu.roll(rp[1], cols - 2 * w, 1)
        )

    def edge_rows(ref, field, k, w):
        for j in range(w):
            ref[0, j, pl.ds(k, 1), :] = field[k, PAD + j:PAD + j + 1, :]
            ref[1, j, pl.ds(k, 1), :] = field[k, PAD + rows - w + j:PAD + rows - w + j + 1, :]

    def send_sums(s, row):
        ar_out[s] = row

        def send(d, carry):
            pltpu.make_async_remote_copy(
                src_ref=ar_out.at[s], dst_ref=ar_in.at[s, d - 1],
                send_sem=as_sem.at[s], recv_sem=ar_sem.at[s],
                device_id=device(d), device_id_type=MESH,
            ).start()
            return carry

        lax.fori_loop(1, n, send, 0)

    def take_sums(s, row):
        pltpu.make_async_copy(ar_in.at[s], ar_in.at[s], ar_sem.at[s]).wait()
        return row + jnp.sum(ar_in[s], axis=0)

    def fold(x):
        return jnp.sum(x.reshape(CHUNK // 8, 8, cols), axis=0)

    def put(row, place, part):
        return jnp.where(lane == place, jnp.sum(part, axis=(0, 1), keepdims=True), row)

    def spread(row):
        for k in range(classes):
            lam_tab[k] = jnp.broadcast_to(
                jnp.sum(jnp.where(lane == k, row, 0.0), axis=1, keepdims=True), (1, cols)
            )

    def offset_of(total, lam):
        return (total - lam * pltpu.roll(total, cols - classes, 1)) * (1.0 / cells)

    def each_class(body, init):
        return lax.fori_loop(0, classes, body, init, unroll=UNROLL)

    starts = range(0, rows, CHUNK)
    zero_row = jnp.zeros((1, cols), jnp.float32)

    load_d.wait()
    load_c.wait()

    def mix(i, carry):
        r = pl.multiple_of(i * 16, 16)
        parts = [d0[j, pl.ds(PAD + r, 16), :] for j in range(classes)]
        for k in range(classes):
            total = src[k, pl.ds(r, 16), :]
            for j in range(classes):
                total = total + coupling[k, j] * parts[j]
            src[k, pl.ds(r, 16), :] = total
        return carry

    lax.fori_loop(0, rows // 16, mix, 0)

    def first(k, row):
        total = jnp.zeros((8, cols), jnp.float32)
        for r0 in starts:
            t = src[k, r0:r0 + CHUNK, :] * 0.5
            u[k, PAD + r0:PAD + r0 + CHUNK, :] = t
            pack(ps.at[1], t, k, r0, 1)
            pack(ps.at[0], d0[k, PAD + r0:PAD + r0 + CHUNK, :], k, r0, 1)
            total = total + fold(t)
        edge_rows(xs.at[1], u, k, 1)
        edge_rows(xs.at[0], d0, k, 1)
        return put(row, k, total)

    row = each_class(first, zero_row)
    pl.semaphore_wait(barrier, n - 1)
    copies = send_halo(1, 1)
    send_sums(0, row)
    dens_copies = send_halo(0, 1)
    sent = [copies, dens_copies]
    lam = zero_row
    own = row

    def neighbours(field, ed, k, r0):
        lo = PAD + r0
        mid = field[k, lo:lo + CHUNK, :]
        xp = field[k, lo + 1:lo + 1 + CHUNK, :]
        xm = field[k, lo - 1:lo - 1 + CHUNK, :]
        side = unpack(ed, k, r0, 1)
        yp = jnp.where(lane_c == cols - 1, side, pltpu.roll(mid, cols - 1, 1))
        ym = jnp.where(lane_c == 0, side, pltpu.roll(mid, 1, 1))
        return xp, xm, yp, ym

    def linear(k, row):
        sum_a = jnp.zeros((8, cols), jnp.float32)
        sum_b = jnp.zeros((8, cols), jnp.float32)
        for r0 in starts:
            xp, xm, yp, ym = neighbours(u, edge, k, r0)
            px = jnp.abs(xp - xm) * 0.5
            py = jnp.abs(yp - ym) * 0.5
            sx, sy = xp + xm, yp + ym
            inv = 1.0 / (2.0 + px + py)
            gain = (sx + sy) + px * (sx - px) + py * (sy - py)
            at_a = (src[k, r0:r0 + CHUNK, :] + 0.5 * gain) * inv
            a[k, r0:r0 + CHUNK, :] = at_a
            b[k, r0:r0 + CHUNK, :] = inv
            sum_a = sum_a + fold(at_a)
            sum_b = sum_b + fold(inv)
        return put(put(row, k, sum_a), classes + k, sum_b)

    for s in range(1, SWEEPS):
        take_halo(copies, s, 1, u)
        row = each_class(linear, zero_row)
        send_sums(s, row)
        total = take_sums(s - 1, own)
        own = row
        offset = offset_of(total, lam)
        lam = THETA * offset
        spread(lam)
        last = s == SWEEPS - 1
        w = 2 if last else 1
        sp, sx = (ps2, xs2) if last else (ps.at[s + 1], xs.at[s + 1])

        def finish(k, carry):
            scale = lam_tab[k]
            for r0 in starts:
                t = a[k, r0:r0 + CHUNK, :] - scale * b[k, r0:r0 + CHUNK, :]
                u[k, PAD + r0:PAD + r0 + CHUNK, :] = t
                pack(sp, t, k, r0, w)
            edge_rows(sx, u, k, w)
            return carry

        each_class(finish, 0)
        copies = send_halo(s + 1, w)
        sent.append(copies)

    out_t = pltpu.make_async_copy(u.at[:, pl.ds(PAD, rows), :], trial_hbm, out_sem.at[0])
    out_t.start()
    take_halo(copies, SWEEPS, 2, u)
    take_halo(dens_copies, 0, 1, d0)

    def flow(field, into, e, c, d, k, r0):
        xp, xm, yp, ym = neighbours(field, edge, k, r0)
        f = c[0] * xp + c[1] * xm + c[2] * yp + c[3] * ym
        into[k, PAD + r0:PAD + r0 + CHUNK, :] = f
        if e is not None:
            pack(ps.at[e], f, k, r0, 1)
            return d
        return d + fold(f)

    base = SWEEPS + 1

    def weigh(k, carry):
        for r0 in starts:
            lo = PAD + r0
            mid = u[k, lo:lo + CHUNK, :]
            xp = u[k, lo + 1:lo + 1 + CHUNK, :]
            xm = u[k, lo - 1:lo - 1 + CHUNK, :]
            xpp = u[k, lo + 2:lo + 2 + CHUNK, :]
            xmm = u[k, lo - 2:lo - 2 + CHUNK, :]
            side = unpack(edge2, k, r0, 2)
            ypp = jnp.where(lane_c >= cols - 2, side, pltpu.roll(mid, cols - 2, 1))
            ymm = jnp.where(lane_c < 2, side, pltpu.roll(mid, 2, 1))
            yp = jnp.where(lane_c == cols - 1, pltpu.roll(side, 1, 1), pltpu.roll(mid, cols - 1, 1))
            ym = jnp.where(lane_c == 0, pltpu.roll(side, cols - 1, 1), pltpu.roll(mid, 1, 1))
            half = 0.5 / (2.0 + 0.5 * (jnp.abs(xp - xm) + jnp.abs(yp - ym)))
            c = [half * (1.0 + jnp.maximum(far - mid, 0.0)) for far in (xpp, xmm, ypp, ymm)]
            for ref, v in zip((cxp, cxm, cyp, cym), c):
                ref[k, r0:r0 + CHUNK, :] = v
            flow(d0, d1, base, c, None, k, r0)
        edge_rows(xs.at[base], d1, k, 1)
        return carry

    each_class(weigh, 0)
    copies = send_halo(base, 1)
    sent.append(copies)

    field, into = d1, d0
    for s in range(1, SWEEPS):
        take_halo(copies, base + s - 1, 1, field)
        last = s == SWEEPS - 1
        e = None if last else base + s

        def sweep(k, row):
            total = jnp.zeros((8, cols), jnp.float32)
            for r0 in starts:
                c = [ref[k, r0:r0 + CHUNK, :] for ref in (cxp, cxm, cyp, cym)]
                total = flow(field, into, e, c, total, k, r0)
            if last:
                return put(row, k, total)
            edge_rows(xs.at[e], into, k, 1)
            return row

        row = each_class(sweep, zero_row)
        if not last:
            copies = send_halo(e, 1)
            sent.append(copies)
        field, into = into, field

    send_sums(SWEEPS, row)
    out_f = pltpu.make_async_copy(field.at[:, pl.ds(PAD, rows), :], fresh_hbm, out_sem.at[1])
    out_f.start()
    total = take_sums(SWEEPS - 1, own)
    means[0:1, :] = offset_of(total, lam)
    for copies in sent:
        for c in copies:
            c.wait_send()
    total = take_sums(SWEEPS, row)
    means[1:2, :] = total * (1.0 / cells)
    for s in range(SWEEPS + 1):
        pltpu.make_async_copy(ar_in.at[s], ar_in.at[s], as_sem.at[s]).wait()
    out_t.wait()
    out_f.wait()


def shards(cost, density_start, coupling):
    nx, ny = lax.axis_size("gx"), lax.axis_size("gy")
    classes, rows, cols = cost.shape
    n = nx * ny
    f32 = jnp.float32
    full = pltpu.VMEM((classes, rows, cols), f32)
    padded = pltpu.VMEM((classes, rows + 2 * PAD, cols), f32)
    slots = 2 * SWEEPS
    block = rows * 2 * classes // cols
    trial, fresh, means = pl.pallas_call(
        functools.partial(kernel, nx, ny),
        out_shape=(
            jax.ShapeDtypeStruct(cost.shape, f32),
            jax.ShapeDtypeStruct(cost.shape, f32),
            jax.ShapeDtypeStruct((2, cols), f32),
        ),
        in_specs=[
            pl.BlockSpec(memory_space=pl.ANY),
            pl.BlockSpec(memory_space=pl.ANY),
            pl.BlockSpec(memory_space=pltpu.SMEM),
        ],
        out_specs=(
            pl.BlockSpec(memory_space=pl.ANY),
            pl.BlockSpec(memory_space=pl.ANY),
            pl.BlockSpec(memory_space=pltpu.VMEM),
        ),
        scratch_shapes=[
            full, padded, full, full, padded, padded, full, full, full, full,
            pltpu.VMEM((slots, 2, 1, classes, cols), f32),
            pltpu.VMEM((slots, 2, 1, classes, cols), f32),
            pltpu.VMEM((slots, block, cols), f32),
            pltpu.VMEM((slots, 2, block, cols), f32),
            pltpu.VMEM((2, 2, classes, cols), f32),
            pltpu.VMEM((2, 2, classes, cols), f32),
            pltpu.VMEM((2 * block, cols), f32),
            pltpu.VMEM((2, 2 * block, cols), f32),
            pltpu.VMEM((block, cols), f32),
            pltpu.VMEM((2 * block, cols), f32),
            pltpu.VMEM((SWEEPS + 1, 1, cols), f32),
            pltpu.VMEM((SWEEPS + 1, n - 1, 1, cols), f32),
            pltpu.VMEM((classes, 1, cols), f32),
            pltpu.SemaphoreType.DMA((2,)),
            pltpu.SemaphoreType.DMA((2,)),
            pltpu.SemaphoreType.DMA((slots, 4)),
            pltpu.SemaphoreType.DMA((slots, 4)),
            pltpu.SemaphoreType.DMA((SWEEPS + 1,)),
            pltpu.SemaphoreType.DMA((SWEEPS + 1,)),
        ],
        compiler_params=pltpu.CompilerParams(
            collective_id=0, has_side_effects=True, vmem_limit_bytes=48 * 1024 * 1024
        ),
    )(cost, density_start, coupling)
    offset = means[0, :classes]
    mass = means[1, :classes]
    value = trial - offset[:, None, None]
    density = fresh / mass[:, None, None]
    return value, density, THETA * offset


def solution(mesh):
    placed = P(None, "gx", "gy")
    return jax.shard_map(
        shards,
        mesh=mesh,
        in_specs=(placed, placed, P()),
        out_specs=(placed, placed, P()),
        check_vma=False,
    )
```

```python
import functools

import jax
import jax.numpy as jnp
from jax import lax
from jax.experimental import pallas as pl
from jax.experimental.pallas import tpu as pltpu
from jax.sharding import PartitionSpec as P

MESH = pl.DeviceIdType.MESH
SWEEPS = 5
THETA = 2.0
PAD = 8
CHUNK = 32
UNROLL = 2


def kernel(
    nx, ny,
    cost_hbm, dens_hbm, coupling,
    trial_hbm, fresh_hbm, means,
    src, u, a, b, d0, d1, cxp, cxm, cyp, cym,
    xs, xr, ps, pr, xs2, xr2, ps2, pr2, edge, edge2, edge3,
    arx_out, arx_in, ary_out, ary_in, lam_tab,
    in_sem, out_sem, hs_sem, hr_sem, axs_sem, axr_sem, ays_sem, ayr_sem,
):
    classes, rows, cols = cost_hbm.shape
    n = nx * ny
    cells = float(n * rows * cols)
    gx, gy = lax.axis_index("gx"), lax.axis_index("gy")
    up, down = lax.rem(gx + nx - 1, nx), lax.rem(gx + 1, nx)
    left, right = lax.rem(gy + ny - 1, ny), lax.rem(gy + 1, ny)

    def at(x, y):
        return {"gx": x, "gy": y}

    peers_x = [at(lax.rem(gx + d, nx), gy) for d in range(1, nx)]
    peers_y = [at(gx, lax.rem(gy + d, ny)) for d in range(1, ny)]

    load_d = pltpu.make_async_copy(dens_hbm, d0.at[:, pl.ds(PAD, rows), :], in_sem.at[0])
    load_c = pltpu.make_async_copy(cost_hbm, src, in_sem.at[1])
    load_d.start()
    load_c.start()

    barrier = pltpu.get_barrier_semaphore()

    for peer in peers_x + peers_y:
        pl.semaphore_signal(barrier, inc=1, device_id=peer, device_id_type=MESH)

    lane = lax.broadcasted_iota(jnp.int32, (1, cols), 1)
    lane_c = lax.broadcasted_iota(jnp.int32, (CHUNK, cols), 1)

    def geometry(w):
        span = 2 * w * classes
        return span, rows // (cols // span)

    def pack(ref, t, k, r0, w):
        span, block = geometry(w)
        p = span * (r0 // block) + 2 * w * k
        q = r0 % block
        turned = pltpu.roll(t, p + w, 1)
        mine = (lane_c >= p) & (lane_c < p + 2 * w)
        ref[q:q + CHUNK, :] = jnp.where(mine, turned, ref[q:q + CHUNK, :])

    def unpack(ref, k, r0, w):
        span, block = geometry(w)
        p = span * (r0 // block) + 2 * w * k
        q = r0 % block
        return pltpu.roll(ref[q:q + CHUNK, :], lax.rem(2 * cols - p, cols), 1)

    def halo_copies(e, w):
        sx, rx, sp, rp = (xs.at[e], xr.at[e], ps.at[e], pr.at[e]) if w == 1 else (xs2, xr2, ps2, pr2)
        plan = (
            (sx.at[0], rx.at[1], at(up, gy)),
            (sx.at[1], rx.at[0], at(down, gy)),
            (sp, rp.at[0], at(gx, right)),
            (sp, rp.at[1], at(gx, left)),
        )
        return [
            pltpu.make_async_remote_copy(
                src_ref=s, dst_ref=r, send_sem=hs_sem.at[e, i], recv_sem=hr_sem.at[e, i],
                device_id=dev, device_id_type=MESH,
            )
            for i, (s, r, dev) in enumerate(plan)
        ]

    def send_halo(e, w):
        copies = halo_copies(e, w)
        for c in copies:
            c.start()
        return copies

    def take_halo(copies, e, w, field):
        for c in copies:
            c.wait_recv()
        rx, rp, ed = (xr.at[e], pr.at[e], edge) if w == 1 else (xr2, pr2, edge2)
        for k in range(classes):
            for j in range(w):
                field[k, PAD - w + j:PAD - w + j + 1, :] = rx[0, j, k:k + 1, :]
                field[k, PAD + rows + j:PAD + rows + j + 1, :] = rx[1, j, k:k + 1, :]
        size = ed.shape[0]
        lanes = lax.broadcasted_iota(jnp.int32, (size, cols), 1)
        ed[...] = jnp.where(
            lax.rem(lanes, 2 * w) < w, rp[0], pltpu.roll(rp[1], cols - 2 * w, 1)
        )

    def edge_rows(ref, field, k, w):
        for j in range(w):
            ref[0, j, pl.ds(k, 1), :] = field[k, PAD + j:PAD + j + 1, :]
            ref[1, j, pl.ds(k, 1), :] = field[k, PAD + rows - w + j:PAD + rows - w + j + 1, :]

    def send_part(s, row, peers, out, into, send_sem, recv_sem):
        out[s] = row
        for i, peer in enumerate(peers):
            pltpu.make_async_remote_copy(
                src_ref=out.at[s], dst_ref=into.at[s, i],
                send_sem=send_sem.at[s], recv_sem=recv_sem.at[s],
                device_id=peer, device_id_type=MESH,
            ).start()

    def send_sums(s, row):
        send_part(s, row, peers_x, arx_out, arx_in, axs_sem, axr_sem)

    def pass_sums(s, row):
        pltpu.make_async_copy(arx_in.at[s], arx_in.at[s], axr_sem.at[s]).wait()
        part = row + jnp.sum(arx_in[s], axis=0)
        send_part(s, part, peers_y, ary_out, ary_in, ays_sem, ayr_sem)
        return part

    def take_sums(s, part):
        pltpu.make_async_copy(ary_in.at[s], ary_in.at[s], ayr_sem.at[s]).wait()
        return part + jnp.sum(ary_in[s], axis=0)

    def fold(x):
        return jnp.sum(x.reshape(CHUNK // 8, 8, cols), axis=0)

    def put(row, place, part):
        return jnp.where(lane == place, jnp.sum(part, axis=(0, 1), keepdims=True), row)

    def spread(row):
        for k in range(classes):
            lam_tab[k] = jnp.broadcast_to(
                jnp.sum(jnp.where(lane == k, row, 0.0), axis=1, keepdims=True), (1, cols)
            )

    def offset_of(total, lam):
        return (total - lam * pltpu.roll(total, cols - classes, 1)) * (1.0 / cells)

    def each_class(body, init):
        return lax.fori_loop(0, classes, body, init, unroll=UNROLL)

    starts = range(0, rows, CHUNK)
    zero_row = jnp.zeros((1, cols), jnp.float32)

    load_d.wait()
    load_c.wait()

    def mix(i, carry):
        r = pl.multiple_of(i * 16, 16)
        parts = [d0[j, pl.ds(PAD + r, 16), :] for j in range(classes)]
        for k in range(classes):
            total = src[k, pl.ds(r, 16), :]
            for j in range(classes):
                total = total + coupling[k, j] * parts[j]
            src[k, pl.ds(r, 16), :] = total
        return carry

    lax.fori_loop(0, rows // 16, mix, 0)

    def first(k, row):
        total = jnp.zeros((8, cols), jnp.float32)
        for r0 in starts:
            t = src[k, r0:r0 + CHUNK, :] * 0.5
            u[k, PAD + r0:PAD + r0 + CHUNK, :] = t
            pack(ps.at[1], t, k, r0, 1)
            pack(ps.at[0], d0[k, PAD + r0:PAD + r0 + CHUNK, :], k, r0, 1)
            total = total + fold(t)
        edge_rows(xs.at[1], u, k, 1)
        edge_rows(xs.at[0], d0, k, 1)
        return put(row, k, total)

    row = each_class(first, zero_row)
    pl.semaphore_wait(barrier, nx + ny - 2)
    copies = send_halo(1, 1)
    send_sums(0, row)
    dens_copies = send_halo(0, 1)
    sent = [copies, dens_copies]
    lam = zero_row
    own = pass_sums(0, row)

    def neighbours(field, ed, k, r0):
        lo = PAD + r0
        mid = field[k, lo:lo + CHUNK, :]
        xp = field[k, lo + 1:lo + 1 + CHUNK, :]
        xm = field[k, lo - 1:lo - 1 + CHUNK, :]
        side = unpack(ed, k, r0, 1)
        yp = jnp.where(lane_c == cols - 1, side, pltpu.roll(mid, cols - 1, 1))
        ym = jnp.where(lane_c == 0, side, pltpu.roll(mid, 1, 1))
        return xp, xm, yp, ym

    def linear(k, row):
        sum_a = jnp.zeros((8, cols), jnp.float32)
        sum_b = jnp.zeros((8, cols), jnp.float32)
        for r0 in starts:
            xp, xm, yp, ym = neighbours(u, edge, k, r0)
            px = jnp.abs(xp - xm) * 0.5
            py = jnp.abs(yp - ym) * 0.5
            sx, sy = xp + xm, yp + ym
            inv = 1.0 / (2.0 + px + py)
            gain = (sx + sy) + px * (sx - px) + py * (sy - py)
            at_a = (src[k, r0:r0 + CHUNK, :] + 0.5 * gain) * inv
            a[k, r0:r0 + CHUNK, :] = at_a
            b[k, r0:r0 + CHUNK, :] = inv
            sum_a = sum_a + fold(at_a)
            sum_b = sum_b + fold(inv)
        return put(put(row, k, sum_a), classes + k, sum_b)

    for s in range(1, SWEEPS):
        take_halo(copies, s, 1, u)
        row = each_class(linear, zero_row)
        send_sums(s, row)
        total = take_sums(s - 1, own)
        offset = offset_of(total, lam)
        lam = THETA * offset
        spread(lam)
        last = s == SWEEPS - 1
        w = 2 if last else 1
        sp, sx = (ps2, xs2) if last else (ps.at[s + 1], xs.at[s + 1])

        def finish(k, carry):
            scale = lam_tab[k]
            for r0 in starts:
                t = a[k, r0:r0 + CHUNK, :] - scale * b[k, r0:r0 + CHUNK, :]
                u[k, PAD + r0:PAD + r0 + CHUNK, :] = t
                pack(sp, t, k, r0, w)
            edge_rows(sx, u, k, w)
            return carry

        each_class(finish, 0)
        copies = send_halo(s + 1, w)
        sent.append(copies)
        own = pass_sums(s, row)

    out_t = pltpu.make_async_copy(u.at[:, pl.ds(PAD, rows), :], trial_hbm, out_sem.at[0])
    out_t.start()
    take_halo(copies, SWEEPS, 2, u)
    take_halo(dens_copies, 0, 1, d0)
    lanes2 = lax.broadcasted_iota(jnp.int32, edge2.shape, 1)
    edge3[...] = jnp.where(
        lax.rem(lanes2, 4) < 2, pltpu.roll(edge2[...], cols - 1, 1), pltpu.roll(edge2[...], 1, 1)
    )

    def flow(field, into, e, c, d, k, r0):
        xp, xm, yp, ym = neighbours(field, edge, k, r0)
        f = c[0] * xp + c[1] * xm + c[2] * yp + c[3] * ym
        into[k, PAD + r0:PAD + r0 + CHUNK, :] = f
        if e is not None:
            pack(ps.at[e], f, k, r0, 1)
            return d
        return d + fold(f)

    base = SWEEPS + 1

    def weigh(k, carry):
        for r0 in starts:
            lo = PAD + r0
            mid = u[k, lo:lo + CHUNK, :]
            xp = u[k, lo + 1:lo + 1 + CHUNK, :]
            xm = u[k, lo - 1:lo - 1 + CHUNK, :]
            xpp = u[k, lo + 2:lo + 2 + CHUNK, :]
            xmm = u[k, lo - 2:lo - 2 + CHUNK, :]
            side = unpack(edge2, k, r0, 2)
            near = unpack(edge3, k, r0, 2)
            ypp = jnp.where(lane_c >= cols - 2, side, pltpu.roll(mid, cols - 2, 1))
            ymm = jnp.where(lane_c < 2, side, pltpu.roll(mid, 2, 1))
            yp = jnp.where(lane_c == cols - 1, near, pltpu.roll(mid, cols - 1, 1))
            ym = jnp.where(lane_c == 0, near, pltpu.roll(mid, 1, 1))
            half = 0.5 / (2.0 + 0.5 * (jnp.abs(xp - xm) + jnp.abs(yp - ym)))
            c = [half * (1.0 + jnp.maximum(far - mid, 0.0)) for far in (xpp, xmm, ypp, ymm)]
            for ref, v in zip((cxp, cxm, cyp, cym), c):
                ref[k, r0:r0 + CHUNK, :] = v
            flow(d0, d1, base, c, None, k, r0)
        edge_rows(xs.at[base], d1, k, 1)
        return carry

    each_class(weigh, 0)
    copies = send_halo(base, 1)
    sent.append(copies)

    field, into = d1, d0
    for s in range(1, SWEEPS):
        take_halo(copies, base + s - 1, 1, field)
        last = s == SWEEPS - 1
        e = None if last else base + s

        def sweep(k, row):
            total = jnp.zeros((8, cols), jnp.float32)
            for r0 in starts:
                c = [ref[k, r0:r0 + CHUNK, :] for ref in (cxp, cxm, cyp, cym)]
                total = flow(field, into, e, c, total, k, r0)
            if last:
                return put(row, k, total)
            edge_rows(xs.at[e], into, k, 1)
            return row

        row = each_class(sweep, zero_row)
        if not last:
            copies = send_halo(e, 1)
            sent.append(copies)
        field, into = into, field

    send_sums(SWEEPS, row)
    out_f = pltpu.make_async_copy(field.at[:, pl.ds(PAD, rows), :], fresh_hbm, out_sem.at[1])
    out_f.start()
    part = pass_sums(SWEEPS, row)
    total = take_sums(SWEEPS - 1, own)
    means[0:1, :] = offset_of(total, lam)
    for copies in sent:
        for c in copies:
            c.wait_send()
    total = take_sums(SWEEPS, part)
    means[1:2, :] = total * (1.0 / cells)
    for s in range(SWEEPS + 1):
        pltpu.make_async_copy(arx_in.at[s], arx_in.at[s], axs_sem.at[s]).wait()
        pltpu.make_async_copy(ary_in.at[s], ary_in.at[s], ays_sem.at[s]).wait()
    out_t.wait()
    out_f.wait()


def shards(cost, density_start, coupling):
    nx, ny = lax.axis_size("gx"), lax.axis_size("gy")
    classes, rows, cols = cost.shape
    f32 = jnp.float32
    full = pltpu.VMEM((classes, rows, cols), f32)
    padded = pltpu.VMEM((classes, rows + 2 * PAD, cols), f32)
    slots = 2 * SWEEPS
    block = rows * 2 * classes // cols
    trial, fresh, means = pl.pallas_call(
        functools.partial(kernel, nx, ny),
        out_shape=(
            jax.ShapeDtypeStruct(cost.shape, f32),
            jax.ShapeDtypeStruct(cost.shape, f32),
            jax.ShapeDtypeStruct((2, cols), f32),
        ),
        in_specs=[
            pl.BlockSpec(memory_space=pl.ANY),
            pl.BlockSpec(memory_space=pl.ANY),
            pl.BlockSpec(memory_space=pltpu.SMEM),
        ],
        out_specs=(
            pl.BlockSpec(memory_space=pl.ANY),
            pl.BlockSpec(memory_space=pl.ANY),
            pl.BlockSpec(memory_space=pltpu.VMEM),
        ),
        scratch_shapes=[
            full, padded, full, full, padded, padded, full, full, full, full,
            pltpu.VMEM((slots, 2, 1, classes, cols), f32),
            pltpu.VMEM((slots, 2, 1, classes, cols), f32),
            pltpu.VMEM((slots, block, cols), f32),
            pltpu.VMEM((slots, 2, block, cols), f32),
            pltpu.VMEM((2, 2, classes, cols), f32),
            pltpu.VMEM((2, 2, classes, cols), f32),
            pltpu.VMEM((2 * block, cols), f32),
            pltpu.VMEM((2, 2 * block, cols), f32),
            pltpu.VMEM((block, cols), f32),
            pltpu.VMEM((2 * block, cols), f32),
            pltpu.VMEM((2 * block, cols), f32),
            pltpu.VMEM((SWEEPS + 1, 1, cols), f32),
            pltpu.VMEM((SWEEPS + 1, nx - 1, 1, cols), f32),
            pltpu.VMEM((SWEEPS + 1, 1, cols), f32),
            pltpu.VMEM((SWEEPS + 1, ny - 1, 1, cols), f32),
            pltpu.VMEM((classes, 1, cols), f32),
            pltpu.SemaphoreType.DMA((2,)),
            pltpu.SemaphoreType.DMA((2,)),
            pltpu.SemaphoreType.DMA((slots, 4)),
            pltpu.SemaphoreType.DMA((slots, 4)),
            pltpu.SemaphoreType.DMA((SWEEPS + 1,)),
            pltpu.SemaphoreType.DMA((SWEEPS + 1,)),
            pltpu.SemaphoreType.DMA((SWEEPS + 1,)),
            pltpu.SemaphoreType.DMA((SWEEPS + 1,)),
        ],
        compiler_params=pltpu.CompilerParams(
            collective_id=0, has_side_effects=True, vmem_limit_bytes=67043328
        ),
    )(cost, density_start, coupling)
    offset = means[0, :classes]
    mass = means[1, :classes]
    value = trial - offset[:, None, None]
    density = fresh / mass[:, None, None]
    return value, density, THETA * offset


def solution(mesh):
    placed = P(None, "gx", "gy")
    return jax.shard_map(
        shards,
        mesh=mesh,
        in_specs=(placed, placed, P()),
        out_specs=(placed, placed, P()),
        check_vma=False,
    )
```

```python
import functools

import jax
import jax.numpy as jnp
from jax import lax
from jax.experimental import pallas as pl
from jax.experimental.pallas import tpu as pltpu
from jax.sharding import PartitionSpec as P

MESH = pl.DeviceIdType.MESH
SWEEPS = 5
THETA = 2.0
PAD = 8
CHUNK = 16
GROUPS = 2
UNROLL = 2


def kernel(
    nx, ny,
    cost_hbm, dens_hbm, coupling,
    trial_hbm, fresh_hbm, means,
    src, u, a, b, d0, d1, cxp, cxm, cyp, cym,
    xs, xr, ps, pr, xs2, xr2, ps2, pr2, edge, edge2, edge3,
    arx_out, arx_in, ary_out, ary_in, lam_tab,
    in_sem, out_sem, hs_sem, hr_sem, axs_sem, axr_sem, ays_sem, ayr_sem,
):
    classes, rows, cols = cost_hbm.shape
    n = nx * ny
    part_of = classes // GROUPS
    cells = float(n * rows * cols)
    gx, gy = lax.axis_index("gx"), lax.axis_index("gy")
    up, down = lax.rem(gx + nx - 1, nx), lax.rem(gx + 1, nx)
    left, right = lax.rem(gy + ny - 1, ny), lax.rem(gy + 1, ny)

    def at(x, y):
        return {"gx": x, "gy": y}

    peers_x = [at(lax.rem(gx + d, nx), gy) for d in range(1, nx)]
    peers_y = [at(gx, lax.rem(gy + d, ny)) for d in range(1, ny)]

    load_d = pltpu.make_async_copy(dens_hbm, d0.at[:, pl.ds(PAD, rows), :], in_sem.at[0])
    load_c = pltpu.make_async_copy(cost_hbm, src, in_sem.at[1])
    load_d.start()
    load_c.start()

    barrier = pltpu.get_barrier_semaphore()

    for peer in peers_x + peers_y:
        pl.semaphore_signal(barrier, inc=1, device_id=peer, device_id_type=MESH)

    lane = lax.broadcasted_iota(jnp.int32, (1, cols), 1)
    lane_c = lax.broadcasted_iota(jnp.int32, (CHUNK, cols), 1)

    def geometry(w):
        span = 2 * w * part_of
        return span, rows // (cols // span)

    def pack(ref, t, k, r0, w):
        span, block = geometry(w)
        p = span * (r0 // block) + 2 * w * lax.rem(k, part_of)
        q = r0 % block
        turned = pltpu.roll(t, p + w, 1)
        mine = (lane_c >= p) & (lane_c < p + 2 * w)
        ref[q:q + CHUNK, :] = jnp.where(mine, turned, ref[q:q + CHUNK, :])

    def unpack(ref, k, r0, w):
        span, block = geometry(w)
        p = span * (r0 // block) + 2 * w * lax.rem(k, part_of)
        q = r0 % block
        return pltpu.roll(ref[q:q + CHUNK, :], lax.rem(2 * cols - p, cols), 1)

    def halo_copies(e, w, g):
        e = e * GROUPS + g
        sx, rx, sp, rp = (xs.at[e], xr.at[e], ps.at[e], pr.at[e]) if w == 1 else (xs2.at[g], xr2.at[g], ps2.at[g], pr2.at[g])
        plan = (
            (sx.at[0], rx.at[1], at(up, gy)),
            (sx.at[1], rx.at[0], at(down, gy)),
            (sp, rp.at[0], at(gx, right)),
            (sp, rp.at[1], at(gx, left)),
        )
        return [
            pltpu.make_async_remote_copy(
                src_ref=s, dst_ref=r, send_sem=hs_sem.at[e, i], recv_sem=hr_sem.at[e, i],
                device_id=dev, device_id_type=MESH,
            )
            for i, (s, r, dev) in enumerate(plan)
        ]

    def send_halo(e, w, g):
        copies = halo_copies(e, w, g)
        for c in copies:
            c.start()
        return copies

    def take_halo(copies, e, w, field, g):
        e = e * GROUPS + g
        for c in copies:
            c.wait_recv()
        rx, rp, ed = (xr.at[e], pr.at[e], edge.at[g]) if w == 1 else (xr2.at[g], pr2.at[g], edge2.at[g])
        for i in range(part_of):
            k = g * part_of + i
            for j in range(w):
                field[k, PAD - w + j:PAD - w + j + 1, :] = rx[0, j, i:i + 1, :]
                field[k, PAD + rows + j:PAD + rows + j + 1, :] = rx[1, j, i:i + 1, :]
        size = ed.shape[0]
        lanes = lax.broadcasted_iota(jnp.int32, (size, cols), 1)
        ed[...] = jnp.where(
            lax.rem(lanes, 2 * w) < w, rp[0], pltpu.roll(rp[1], cols - 2 * w, 1)
        )

    def edge_rows(ref, field, k, w):
        i = lax.rem(k, part_of)
        for j in range(w):
            ref[0, j, pl.ds(i, 1), :] = field[k, PAD + j:PAD + j + 1, :]
            ref[1, j, pl.ds(i, 1), :] = field[k, PAD + rows - w + j:PAD + rows - w + j + 1, :]

    def send_part(s, row, peers, out, into, send_sem, recv_sem):
        out[s] = row
        for i, peer in enumerate(peers):
            pltpu.make_async_remote_copy(
                src_ref=out.at[s], dst_ref=into.at[s, i],
                send_sem=send_sem.at[s], recv_sem=recv_sem.at[s],
                device_id=peer, device_id_type=MESH,
            ).start()

    def send_sums(s, row):
        send_part(s, row, peers_x, arx_out, arx_in, axs_sem, axr_sem)

    def pass_sums(s, row):
        pltpu.make_async_copy(arx_in.at[s], arx_in.at[s], axr_sem.at[s]).wait()
        part = row + jnp.sum(arx_in[s], axis=0)
        send_part(s, part, peers_y, ary_out, ary_in, ays_sem, ayr_sem)
        return part

    def take_sums(s, part):
        pltpu.make_async_copy(ary_in.at[s], ary_in.at[s], ayr_sem.at[s]).wait()
        return part + jnp.sum(ary_in[s], axis=0)

    def fold(x):
        return jnp.sum(x.reshape(CHUNK // 8, 8, cols), axis=0)

    def put(row, place, part):
        return jnp.where(lane == place, jnp.sum(part, axis=(0, 1), keepdims=True), row)

    def spread(row, g):
        for k in range(g * part_of, (g + 1) * part_of):
            lam_tab[k] = jnp.broadcast_to(
                jnp.sum(jnp.where(lane == k, row, 0.0), axis=1, keepdims=True), (1, cols)
            )

    def offset_of(total, lam):
        return (total - lam * pltpu.roll(total, cols - classes, 1)) * (1.0 / cells)

    def each_class(g, body, init):
        return lax.fori_loop(g * part_of, (g + 1) * part_of, body, init, unroll=UNROLL)

    starts = range(0, rows, CHUNK)
    zero_row = jnp.zeros((1, cols), jnp.float32)

    load_d.wait()
    load_c.wait()

    def mix(i, carry):
        r = pl.multiple_of(i * 16, 16)
        parts = [d0[j, pl.ds(PAD + r, 16), :] for j in range(classes)]
        for k in range(classes):
            total = src[k, pl.ds(r, 16), :]
            for j in range(classes):
                total = total + coupling[k, j] * parts[j]
            src[k, pl.ds(r, 16), :] = total
        return carry

    lax.fori_loop(0, rows // 16, mix, 0)

    def first(g, k, row):
        total = jnp.zeros((8, cols), jnp.float32)
        for r0 in starts:
            t = src[k, r0:r0 + CHUNK, :] * 0.5
            u[k, PAD + r0:PAD + r0 + CHUNK, :] = t
            pack(ps.at[GROUPS + g], t, k, r0, 1)
            pack(ps.at[g], d0[k, PAD + r0:PAD + r0 + CHUNK, :], k, r0, 1)
            total = total + fold(t)
        edge_rows(xs.at[GROUPS + g], u, k, 1)
        edge_rows(xs.at[g], d0, k, 1)
        return put(row, k, total)

    copies, dens_copies, rows_of, own, sent = {}, {}, {}, {}, []
    lam = {g: zero_row for g in range(GROUPS)}
    pending = []

    def settle():
        while pending:
            s, g = pending.pop(0)
            own[g] = pass_sums(s * GROUPS + g, rows_of[g])

    for g in range(GROUPS):
        rows_of[g] = each_class(g, functools.partial(first, g), zero_row)
        if g == 0:
            pl.semaphore_wait(barrier, nx + ny - 2)
        copies[g] = send_halo(1, 1, g)
        send_sums(g, rows_of[g])
        dens_copies[g] = send_halo(0, 1, g)
        sent += [copies[g], dens_copies[g]]
        pending.append((0, g))

    def neighbours(field, ed, k, r0):
        lo = PAD + r0
        mid = field[k, lo:lo + CHUNK, :]
        xp = field[k, lo + 1:lo + 1 + CHUNK, :]
        xm = field[k, lo - 1:lo - 1 + CHUNK, :]
        side = unpack(ed, k, r0, 1)
        yp = jnp.where(lane_c == cols - 1, side, pltpu.roll(mid, cols - 1, 1))
        ym = jnp.where(lane_c == 0, side, pltpu.roll(mid, 1, 1))
        return xp, xm, yp, ym

    def linear(g, k, row):
        sum_a = jnp.zeros((8, cols), jnp.float32)
        sum_b = jnp.zeros((8, cols), jnp.float32)
        for r0 in starts:
            xp, xm, yp, ym = neighbours(u, edge.at[g], k, r0)
            px = jnp.abs(xp - xm) * 0.5
            py = jnp.abs(yp - ym) * 0.5
            sx, sy = xp + xm, yp + ym
            inv = 1.0 / (2.0 + px + py)
            gain = (sx + sy) + px * (sx - px) + py * (sy - py)
            at_a = (src[k, r0:r0 + CHUNK, :] + 0.5 * gain) * inv
            a[k, r0:r0 + CHUNK, :] = at_a
            b[k, r0:r0 + CHUNK, :] = inv
            sum_a = sum_a + fold(at_a)
            sum_b = sum_b + fold(inv)
        return put(put(row, k, sum_a), classes + k, sum_b)

    for s in range(1, SWEEPS):
        last = s == SWEEPS - 1
        w = 2 if last else 1
        for g in range(GROUPS):
            take_halo(copies[g], s, 1, u, g)
            settle()
            row = each_class(g, functools.partial(linear, g), zero_row)
            send_sums(s * GROUPS + g, row)
            total = take_sums((s - 1) * GROUPS + g, own[g])
            lam[g] = THETA * offset_of(total, lam[g])
            spread(lam[g], g)
            rows_of[g] = row
            slot = (s + 1) * GROUPS + g
            sp, sx = (ps2.at[g], xs2.at[g]) if last else (ps.at[slot], xs.at[slot])

            def finish(k, carry):
                scale = lam_tab[k]
                for r0 in starts:
                    t = a[k, r0:r0 + CHUNK, :] - scale * b[k, r0:r0 + CHUNK, :]
                    u[k, PAD + r0:PAD + r0 + CHUNK, :] = t
                    pack(sp, t, k, r0, w)
                edge_rows(sx, u, k, w)
                return carry

            each_class(g, finish, 0)
            copies[g] = send_halo(s + 1, w, g)
            sent.append(copies[g])
            pending.append((s, g))

    out_t = pltpu.make_async_copy(u.at[:, pl.ds(PAD, rows), :], trial_hbm, out_sem.at[0])
    out_t.start()
    def flow(field, into, e, c, d, g, k, r0):
        xp, xm, yp, ym = neighbours(field, edge.at[g], k, r0)
        f = c[0] * xp + c[1] * xm + c[2] * yp + c[3] * ym
        into[k, PAD + r0:PAD + r0 + CHUNK, :] = f
        if e is not None:
            pack(ps.at[e * GROUPS + g], f, k, r0, 1)
            return d
        return d + fold(f)

    base = SWEEPS + 1

    def weigh(g, k, carry):
        for r0 in starts:
            lo = PAD + r0
            mid = u[k, lo:lo + CHUNK, :]
            xp = u[k, lo + 1:lo + 1 + CHUNK, :]
            xm = u[k, lo - 1:lo - 1 + CHUNK, :]
            xpp = u[k, lo + 2:lo + 2 + CHUNK, :]
            xmm = u[k, lo - 2:lo - 2 + CHUNK, :]
            side = unpack(edge2.at[g], k, r0, 2)
            near = unpack(edge3.at[g], k, r0, 2)
            ypp = jnp.where(lane_c >= cols - 2, side, pltpu.roll(mid, cols - 2, 1))
            ymm = jnp.where(lane_c < 2, side, pltpu.roll(mid, 2, 1))
            yp = jnp.where(lane_c == cols - 1, near, pltpu.roll(mid, cols - 1, 1))
            ym = jnp.where(lane_c == 0, near, pltpu.roll(mid, 1, 1))
            half = 0.5 / (2.0 + 0.5 * (jnp.abs(xp - xm) + jnp.abs(yp - ym)))
            c = [half * (1.0 + jnp.maximum(far - mid, 0.0)) for far in (xpp, xmm, ypp, ymm)]
            for ref, v in zip((cxp, cxm, cyp, cym), c):
                ref[k, r0:r0 + CHUNK, :] = v
            flow(d0, d1, base, c, None, g, k, r0)
        edge_rows(xs.at[base * GROUPS + g], d1, k, 1)
        return carry

    for g in range(GROUPS):
        take_halo(copies[g], SWEEPS, 2, u, g)
        settle()
        take_halo(dens_copies[g], 0, 1, d0, g)
        far = edge2[g]
        lanes2 = lax.broadcasted_iota(jnp.int32, far.shape, 1)
        edge3[g] = jnp.where(
            lax.rem(lanes2, 4) < 2, pltpu.roll(far, cols - 1, 1), pltpu.roll(far, 1, 1)
        )
        each_class(g, functools.partial(weigh, g), 0)
        copies[g] = send_halo(base, 1, g)
        sent.append(copies[g])

    field, into = d1, d0
    for s in range(1, SWEEPS):
        last = s == SWEEPS - 1
        e = None if last else base + s
        for g in range(GROUPS):
            take_halo(copies[g], base + s - 1, 1, field, g)

            def sweep(k, row):
                total = jnp.zeros((8, cols), jnp.float32)
                for r0 in starts:
                    c = [ref[k, r0:r0 + CHUNK, :] for ref in (cxp, cxm, cyp, cym)]
                    total = flow(field, into, e, c, total, g, k, r0)
                if last:
                    return put(row, k, total)
                edge_rows(xs.at[e * GROUPS + g], into, k, 1)
                return row

            rows_of[g] = each_class(g, sweep, zero_row)
            if last:
                send_sums(SWEEPS * GROUPS + g, rows_of[g])
            else:
                copies[g] = send_halo(e, 1, g)
                sent.append(copies[g])
        field, into = into, field

    out_f = pltpu.make_async_copy(field.at[:, pl.ds(PAD, rows), :], fresh_hbm, out_sem.at[1])
    out_f.start()
    means[0:1, :] = sum(
        offset_of(take_sums((SWEEPS - 1) * GROUPS + g, own[g]), lam[g]) for g in range(GROUPS)
    )
    pending += [(SWEEPS, g) for g in range(GROUPS)]
    settle()
    for copies in sent:
        for c in copies:
            c.wait_send()
    total = sum(take_sums(SWEEPS * GROUPS + g, own[g]) for g in range(GROUPS))
    means[1:2, :] = total * (1.0 / cells)
    for s in range((SWEEPS + 1) * GROUPS):
        pltpu.make_async_copy(arx_in.at[s], arx_in.at[s], axs_sem.at[s]).wait()
        pltpu.make_async_copy(ary_in.at[s], ary_in.at[s], ays_sem.at[s]).wait()
    out_t.wait()
    out_f.wait()


def shards(cost, density_start, coupling):
    nx, ny = lax.axis_size("gx"), lax.axis_size("gy")
    classes, rows, cols = cost.shape
    f32 = jnp.float32
    full = pltpu.VMEM((classes, rows, cols), f32)
    padded = pltpu.VMEM((classes, rows + 2 * PAD, cols), f32)
    slots = 2 * SWEEPS * GROUPS
    some = classes // GROUPS
    sums = (SWEEPS + 1) * GROUPS
    block = rows * 2 * some // cols
    trial, fresh, means = pl.pallas_call(
        functools.partial(kernel, nx, ny),
        out_shape=(
            jax.ShapeDtypeStruct(cost.shape, f32),
            jax.ShapeDtypeStruct(cost.shape, f32),
            jax.ShapeDtypeStruct((2, cols), f32),
        ),
        in_specs=[
            pl.BlockSpec(memory_space=pl.ANY),
            pl.BlockSpec(memory_space=pl.ANY),
            pl.BlockSpec(memory_space=pltpu.SMEM),
        ],
        out_specs=(
            pl.BlockSpec(memory_space=pl.ANY),
            pl.BlockSpec(memory_space=pl.ANY),
            pl.BlockSpec(memory_space=pltpu.VMEM),
        ),
        scratch_shapes=[
            full, padded, full, full, padded, padded, full, full, full, full,
            pltpu.VMEM((slots, 2, 1, some, cols), f32),
            pltpu.VMEM((slots, 2, 1, some, cols), f32),
            pltpu.VMEM((slots, block, cols), f32),
            pltpu.VMEM((slots, 2, block, cols), f32),
            pltpu.VMEM((GROUPS, 2, 2, some, cols), f32),
            pltpu.VMEM((GROUPS, 2, 2, some, cols), f32),
            pltpu.VMEM((GROUPS, 2 * block, cols), f32),
            pltpu.VMEM((GROUPS, 2, 2 * block, cols), f32),
            pltpu.VMEM((GROUPS, block, cols), f32),
            pltpu.VMEM((GROUPS, 2 * block, cols), f32),
            pltpu.VMEM((GROUPS, 2 * block, cols), f32),
            pltpu.VMEM((sums, 1, cols), f32),
            pltpu.VMEM((sums, nx - 1, 1, cols), f32),
            pltpu.VMEM((sums, 1, cols), f32),
            pltpu.VMEM((sums, ny - 1, 1, cols), f32),
            pltpu.VMEM((classes, 1, cols), f32),
            pltpu.SemaphoreType.DMA((2,)),
            pltpu.SemaphoreType.DMA((2,)),
            pltpu.SemaphoreType.DMA((slots, 4)),
            pltpu.SemaphoreType.DMA((slots, 4)),
            pltpu.SemaphoreType.DMA((sums,)),
            pltpu.SemaphoreType.DMA((sums,)),
            pltpu.SemaphoreType.DMA((sums,)),
            pltpu.SemaphoreType.DMA((sums,)),
        ],
        compiler_params=pltpu.CompilerParams(
            collective_id=0, has_side_effects=True, vmem_limit_bytes=67043328
        ),
    )(cost, density_start, coupling)
    offset = means[0, :classes]
    mass = means[1, :classes]
    value = trial - offset[:, None, None]
    density = fresh / mass[:, None, None]
    return value, density, THETA * offset


def solution(mesh):
    placed = P(None, "gx", "gy")
    return jax.shard_map(
        shards,
        mesh=mesh,
        in_specs=(placed, placed, P()),
        out_specs=(placed, placed, P()),
        check_vma=False,
    )
```
